256 devices in a mesh: shard: 32 (over z_lo, y, core), model: 8 (over z_hi, x).
Axes of the slice: x: 4, y: 4, z: 8 (z_hi: 2, z_lo: 4; z = z_hi * 4 + z_lo), core: 2. Of those that a mesh axis runs over, the one named last changes fastest.
Arguments:
- gradients: float32 [256, 128, 4096], P(None, 'shard', 'model'), may hold values from -6 to 6
- momentum: float32 [256, 128, 4096], P(None, 'shard', 'model'), may hold values from -6 to 6
- weights: float32 [256, 128, 4096], P(None, 'shard', 'model'), may hold values from -0.1875 to 0.1875
Outputs:
- new_weights: float32 [256, 128, 4096], P(None, 'shard', 'model')
- new_momentum: float32 [256, 128, 4096], P(None, 'shard', 'model')
The draws below stay inside these ranges and needn't reach their ends.
All inputs are finite; a program needn't handle non-finite values.
Results may differ from the reference program's by a relative error of at most 0.00012.
Values sent between devices are 32-bit elements; how exact they have to be, the bound alone decides.
No kernel may reach another device: no remote copies, remote signals or barrier semaphores. Data moves between devices by JAX's collectives and lax.ppermute only.
A program may use at most 64 MiB of HBM per device.

```python
import jax
import jax.numpy as jnp
from jax import lax

SIDE = 128
WIDE = 4096
MATS = 256
ITERS = 4


def steps_of(key, dims, pieces, smallest, top_value):
    level = 1.0
    for dim, parts in pieces:
        heights = jax.random.uniform(jax.random.fold_in(jax.random.fold_in(key, 6), dim), (parts,), jnp.float32, smallest / len(pieces), top_value / len(pieces))
        level = level * jnp.repeat(jnp.exp(heights), dims[dim] // parts).reshape((-1,) + (1,) * (len(dims) - 1 - dim))
    return level


def gaussian(stream_key, dims, width, bound, split=(), kind=jnp.bfloat16):
    result = jax.random.normal(stream_key, dims, jnp.float32) * width
    if len(split) > 0:
        result = steps_of(stream_key, dims, split, -0.22, 0.18) * result
    return jnp.clip(result, min=-bound, max=bound).astype(kind)


def setup_inputs(seed: int = 0) -> dict:
    keys = jax.random.split(jax.random.key(seed), 4)
    return {
        "gradients": gaussian(keys[0], (MATS, SIDE, WIDE), 1.0, 6.0, ((1, 32), (2, 8)), jnp.float32),
        "momentum": gaussian(keys[1], (MATS, SIDE, WIDE), 1.0, 6.0, ((1, 32), (2, 8)), jnp.float32),
        "weights": gaussian(keys[2], (MATS, SIDE, WIDE), 0.03, 0.1875, ((1, 32), (2, 8)), jnp.float32),
    }


hold_rate = 0.9
learn_rate = 0.8

def reference(gradients, momentum, weights):
    new_momentum = hold_rate * momentum + gradients
    direction = hold_rate * new_momentum + gradients

    def orthogonal_one(stack):
        iterate = stack[None]
        iterate = iterate * lax.rsqrt(lax.optimization_barrier(jnp.sum(iterate * iterate, axis=(1, 2), keepdims=True)) + 1e-06)
        for step in range(ITERS):
            gram = jnp.einsum('mik,mjk->mij', iterate, iterate, precision=lax.Precision.HIGHEST)
            mixed = -4.775 * gram + 2.0315 * jnp.einsum('mij,mjk->mik', gram, gram, precision=lax.Precision.HIGHEST)
            iterate = 3.4445 * iterate + jnp.einsum('mij,mjk->mik', mixed, iterate, precision=lax.Precision.HIGHEST)
        return iterate[0]
    iterate = lax.map(orthogonal_one, direction)
    new_weights = weights - learn_rate * iterate
    return (new_weights, new_momentum)
```

```python
import jax
import jax.numpy as jnp
from jax import lax
from jax.experimental import pallas as pl
from jax.experimental.pallas import tpu as pltpu
from jax.sharding import Mesh
from jax.sharding import PartitionSpec as P

ITERS = 4
SHARD = ("shard_0", "shard_1", "shard_2")
HIGH = lax.Precision.HIGHEST

hold_rate = 0.9
learn_rate = 0.8


def dot(a, b):
    return jnp.dot(a, b, precision=HIGH, preferred_element_type=jnp.float32)


def gram_body(x_ref, out_ref):
    x = x_ref[:, 0].reshape(128, x_ref.shape[-1])
    out_ref[0] = lax.dot_general(x, x, (((1,), (1,)), ((), ())), precision=HIGH, preferred_element_type=jnp.float32)


def grams(x):
    sources, mats, rows, wide = x.shape
    side = sources * rows
    return pl.pallas_call(
        gram_body,
        grid=(mats,),
        in_specs=[pl.BlockSpec((sources, 1, rows, wide), lambda i: (0, i, 0, 0))],
        out_specs=pl.BlockSpec((1, side, side), lambda i: (i, 0, 0)),
        out_shape=jax.ShapeDtypeStruct((mats, side, side), jnp.float32),
    )(x)


def chain_body(mine_ref, theirs_ref, out_ref):
    side = out_ref.shape[-1]
    row = lax.broadcasted_iota(jnp.int32, (side, side), 0)
    col = lax.broadcasted_iota(jnp.int32, (side, side), 1)
    eye = jnp.where(row == col, 1.0, 0.0)
    for i in range(out_ref.shape[0]):
        gram = mine_ref[i] + theirs_ref[i]
        scale = lax.rsqrt(jnp.sum(gram * eye, keepdims=True) + 1e-06)
        a = gram * (scale * scale)
        q = None
        for step in range(ITERS):
            p = 3.4445 * eye + (-4.775 * a + 2.0315 * dot(a, a))
            q = p * scale if q is None else dot(p, q)
            if step + 1 < ITERS:
                a = dot(p, dot(p, a))
        out_ref[i] = q


def chain(mine, theirs):
    return pl.pallas_call(
        chain_body,
        out_shape=jax.ShapeDtypeStruct(mine.shape, jnp.float32),
    )(mine, theirs)


def apply_body(q_ref, x_ref, out_ref):
    sources, _, rows, wide = x_ref.shape
    x = x_ref[:, 0].reshape(sources * rows, wide)
    out_ref[:, 0] = dot(q_ref[0], x).reshape(sources, rows, wide)


def applied(q, x):
    sources, mats, rows, wide = x.shape
    side = sources * rows
    block = pl.BlockSpec((sources, 1, rows, wide), lambda i: (0, i, 0, 0))
    return pl.pallas_call(
        apply_body,
        grid=(mats,),
        in_specs=[pl.BlockSpec((1, side, side), lambda i: (i, 0, 0)), block],
        out_specs=block,
        out_shape=jax.ShapeDtypeStruct(x.shape, jnp.float32),
    )(q, x)


def local(gradients, momentum, weights):
    new_momentum = hold_rate * momentum + gradients
    direction = hold_rate * new_momentum + gradients
    group = lax.axis_size(SHARD)
    mats, rows, wide = direction.shape
    across = lax.axis_size("x")
    x = lax.all_to_all(direction.reshape(group, mats // group, rows, wide), SHARD, 0, 0, tiled=True)
    part = grams(x)
    side = part.shape[-1]
    part = lax.all_to_all(part.reshape(across, -1, side, side), "x", 0, 0, tiled=True)
    mine = jnp.sum(part, axis=0)
    theirs = lax.ppermute(mine, "z_hi", [(0, 1), (1, 0)])
    q = chain(mine, theirs)
    q = lax.all_to_all(jnp.broadcast_to(q[None], (across, *q.shape)), "x", 0, 0, tiled=True)
    y = applied(q.reshape(-1, side, side), x)
    back = lax.all_to_all(y, SHARD, 0, 0, tiled=True).reshape(mats, rows, wide)
    return (weights - learn_rate * back, new_momentum)


def solution(mesh):
    finer = Mesh(
        mesh.devices.reshape(4, 4, 2, 2, 4),
        ("shard_0", "shard_1", "shard_2", "z_hi", "x"),
    )
    placed = P(None, SHARD, ("z_hi", "x"))
    return jax.shard_map(
        local,
        mesh=finer,
        in_specs=(placed, placed, placed),
        out_specs=(placed, placed),
        check_vma=False,
    )
```

```python
import jax
import jax.numpy as jnp
from jax import lax
from jax.experimental import pallas as pl
from jax.experimental.pallas import tpu as pltpu
from jax.sharding import Mesh
from jax.sharding import PartitionSpec as P

ITERS = 4
SHARD = ("shard_0", "shard_1", "shard_2")
HIGH = lax.Precision.HIGHEST

hold_rate = 0.9
learn_rate = 0.8


def dot(a, b):
    return jnp.dot(a, b, precision=HIGH, preferred_element_type=jnp.float32)


def polynomial(gram):
    side = gram.shape[-1]
    row = lax.broadcasted_iota(jnp.int32, (side, side), 0)
    col = lax.broadcasted_iota(jnp.int32, (side, side), 1)
    eye = jnp.where(row == col, 1.0, 0.0)
    scale = lax.rsqrt(jnp.sum(gram * eye, keepdims=True) + 1e-06)
    a = gram * (scale * scale)
    q = None
    for step in range(ITERS):
        p = 3.4445 * eye + (-4.775 * a + 2.0315 * dot(a, a))
        q = p * scale if q is None else dot(p, q)
        if step + 1 < ITERS:
            a = dot(p, dot(p, a))
    return q


def update_body(x_ref, out_ref):
    sources, parts, rows, wide = x_ref.shape
    side = sources * rows
    gram = None
    for part in range(parts):
        x = x_ref[:, part].reshape(side, wide)
        product = lax.dot_general(x, x, (((1,), (1,)), ((), ())), precision=HIGH, preferred_element_type=jnp.float32)
        gram = product if gram is None else gram + product
    q = polynomial(gram)
    for part in range(parts):
        x = x_ref[:, part].reshape(side, wide)
        out_ref[:, part] = dot(q, x).reshape(sources, rows, wide)


def updated(x):
    return pl.pallas_call(
        update_body,
        in_specs=[pl.BlockSpec(memory_space=pltpu.VMEM)],
        out_specs=pl.BlockSpec(memory_space=pltpu.VMEM),
        out_shape=jax.ShapeDtypeStruct(x.shape, jnp.float32),
    )(x)


def local(gradients, momentum, weights):
    new_momentum = hold_rate * momentum + gradients
    direction = hold_rate * new_momentum + gradients
    mats, rows, wide = direction.shape
    sources = lax.axis_size(SHARD)
    every = (*SHARD, "model")
    x = lax.all_to_all(direction, every, 0, 0, tiled=True)
    y = updated(x.reshape(sources, -1, rows, wide))
    back = lax.all_to_all(y.reshape(mats, rows, wide), every, 0, 0, tiled=True)
    return (weights - learn_rate * back, new_momentum)


def solution(mesh):
    finer = Mesh(
        mesh.devices.reshape(4, 4, 2, mesh.shape["model"]),
        (*SHARD, "model"),
    )
    placed = P(None, SHARD, "model")
    return jax.shard_map(
        local,
        mesh=finer,
        in_specs=(placed, placed, placed),
        out_specs=(placed, placed),
        check_vma=False,
    )
```

```python
import jax
import jax.numpy as jnp
from jax import lax
from jax.experimental import pallas as pl
from jax.experimental.pallas import tpu as pltpu
from jax.sharding import Mesh
from jax.sharding import PartitionSpec as P

ITERS = 4
SHARD = ("shard_0", "shard_1", "shard_2")

hold_rate = 0.9
learn_rate = 0.8


STEPS = 8


def direction_body(gradients_ref, momentum_ref, out_ref, new_ref, first_ref, second_ref, arrived):
    step = out_ref.shape[0] // STEPS

    def copies(i):
        rows = pl.ds(i * step, step)
        return (
            pltpu.make_async_copy(gradients_ref.at[rows], first_ref.at[rows], arrived.at[0, i]),
            pltpu.make_async_copy(momentum_ref.at[rows], second_ref.at[rows], arrived.at[1, i]),
        )

    for i in range(STEPS):
        for copy in copies(i):
            copy.start()
    for i in range(STEPS):
        for copy in copies(i):
            copy.wait()
        rows = pl.ds(i * step, step)
        gradients = first_ref[rows]
        new_momentum = hold_rate * second_ref[rows] + gradients
        new_ref[rows] = new_momentum
        out_ref[rows] = hold_rate * new_momentum + gradients


def direction_of(gradients, momentum):
    whole = pltpu.VMEM(gradients.shape, gradients.dtype)
    return pl.pallas_call(
        direction_body,
        in_specs=[pl.BlockSpec(memory_space=pltpu.HBM), pl.BlockSpec(memory_space=pltpu.HBM)],
        out_specs=[pl.BlockSpec(memory_space=pltpu.VMEM), pl.BlockSpec(memory_space=pltpu.VMEM)],
        out_shape=[whole, whole],
        scratch_shapes=[whole, whole, pltpu.SemaphoreType.DMA((2, STEPS))],
        compiler_params=pltpu.CompilerParams(vmem_limit_bytes=16 << 20),
    )(pltpu.with_memory_space_constraint(gradients, pltpu.HBM), pltpu.with_memory_space_constraint(momentum, pltpu.HBM))


def in_parts(x):
    first = x.astype(jnp.bfloat16)
    rest = x - first.astype(jnp.float32)
    second = rest.astype(jnp.bfloat16)
    third = (rest - second.astype(jnp.float32)).astype(jnp.bfloat16)
    return first, second, third


def on_left(a):
    first, second, third = in_parts(a)
    return jnp.concatenate([first, first, second, second, first, third], axis=1)


def on_right(b):
    first, second, third = in_parts(b)
    return jnp.concatenate([first, second, first, second, third, first], axis=0)


def product(left, right):
    return jnp.dot(left, right, preferred_element_type=jnp.float32)


def polynomial(gram):
    side = gram.shape[-1]
    row = lax.broadcasted_iota(jnp.int32, (side, side), 0)
    col = lax.broadcasted_iota(jnp.int32, (side, side), 1)
    eye = jnp.where(row == col, 1.0, 0.0)
    scale = lax.rsqrt(jnp.sum(gram * eye, keepdims=True) + 1e-06)
    a = gram * (scale * scale)
    q = eye * scale
    for step in range(ITERS):
        square = product(on_left(a), on_right(a))
        p = 3.4445 * eye + (-4.775 * a + 2.0315 * square)
        if step + 1 == ITERS:
            return product(on_left(p), on_right(q))
        left = on_left(p)
        if step == 0:
            q = p * scale
            once = product(left, on_right(a))
        else:
            both = product(left, on_right(jnp.concatenate([a, q], axis=1)))
            once, q = both[:, :side], both[:, side:]
        a = product(left, on_right(once))


def update_body(x_ref, momentum_ref, out_ref, kept_ref, written):
    keep = pltpu.make_async_copy(momentum_ref, kept_ref, written)
    keep.start()
    sources, parts, rows, wide = x_ref.shape
    side = sources * rows
    sums = None
    for part in range(parts):
        x = x_ref[:, part].reshape(side, wide)
        pieces = jnp.concatenate(in_parts(x), axis=0)
        new = lax.dot_general(
            pieces, pieces[: 2 * side], (((1,), (1,)), ((), ())), preferred_element_type=jnp.float32
        )
        sums = new if sums is None else sums + new
    small = sums[2 * side :, :side]
    small = (small + small.T) + sums[side : 2 * side, side:]
    small = small + (sums[side : 2 * side, :side] + sums[:side, side:])
    q = on_left(polynomial(sums[:side, :side] + small))
    for part in range(parts):
        x = x_ref[:, part].reshape(side, wide)
        out_ref[:, part] = product(q, on_right(x)).reshape(sources, rows, wide)
    keep.wait()


def updated(x, momentum):
    return pl.pallas_call(
        update_body,
        in_specs=[pl.BlockSpec(memory_space=pltpu.VMEM), pl.BlockSpec(memory_space=pltpu.VMEM)],
        out_specs=[pl.BlockSpec(memory_space=pltpu.VMEM), pl.BlockSpec(memory_space=pltpu.HBM)],
        out_shape=[pltpu.VMEM(x.shape, x.dtype), pltpu.HBM(momentum.shape, momentum.dtype)],
        scratch_shapes=[pltpu.SemaphoreType.DMA],
        compiler_params=pltpu.CompilerParams(vmem_limit_bytes=16 << 20),
    )(pltpu.with_memory_space_constraint(x, pltpu.VMEM), pltpu.with_memory_space_constraint(momentum, pltpu.VMEM))


def local(gradients, momentum, weights):
    direction, new_momentum = direction_of(gradients, momentum)
    mats, rows, wide = direction.shape
    sources = lax.axis_size(SHARD)
    every = (*SHARD, "model")
    x = lax.all_to_all(direction, every, 0, 0, tiled=True)
    y, new_momentum = updated(x.reshape(sources, -1, rows, wide), new_momentum)
    back = lax.all_to_all(y.reshape(mats, rows, wide), every, 0, 0, tiled=True)
    return (weights - learn_rate * back, new_momentum)


def solution(mesh):
    finer = Mesh(
        mesh.devices.reshape(4, 4, 2, mesh.shape["model"]),
        (*SHARD, "model"),
    )
    placed = P(None, SHARD, "model")
    return jax.shard_map(
        local,
        mesh=finer,
        in_specs=(placed, placed, placed),
        out_specs=(placed, placed),
        check_vma=False,
    )
```

```python
import jax
import jax.numpy as jnp
from jax import lax
from jax.experimental import pallas as pl
from jax.experimental.pallas import tpu as pltpu
from jax.sharding import Mesh
from jax.sharding import PartitionSpec as P

ITERS = 4
SHARD = ("shard_0", "shard_1", "shard_2")
MODEL = ("model_0", "model_1")
EVERY = ("shard_2", "model_0", "shard_0", "shard_1", "model_1")
STEPS = 8

hold_rate = 0.9
learn_rate = 0.8

limits = pltpu.CompilerParams(vmem_limit_bytes=16 << 20)


def direction_body(gradients_ref, momentum_ref, out_ref, new_ref, first_ref, second_ref, arrived):
    step = out_ref.shape[0] // STEPS

    def copies(i):
        rows = pl.ds(i * step, step)
        return (
            pltpu.make_async_copy(gradients_ref.at[rows], first_ref.at[rows], arrived.at[0, i]),
            pltpu.make_async_copy(momentum_ref.at[rows], second_ref.at[rows], arrived.at[1, i]),
        )

    for i in range(STEPS):
        for copy in copies(i):
            copy.start()
    for i in range(STEPS):
        for copy in copies(i):
            copy.wait()
        rows = pl.ds(i * step, step)
        gradients = first_ref[rows]
        new_momentum = hold_rate * second_ref[rows] + gradients
        new_ref[rows] = new_momentum
        out_ref[rows] = hold_rate * new_momentum + gradients


def direction_of(gradients, momentum):
    whole = pltpu.VMEM(gradients.shape, gradients.dtype)
    return pl.pallas_call(
        direction_body,
        in_specs=[pl.BlockSpec(memory_space=pltpu.HBM), pl.BlockSpec(memory_space=pltpu.HBM)],
        out_specs=[pl.BlockSpec(memory_space=pltpu.VMEM), pl.BlockSpec(memory_space=pltpu.VMEM)],
        out_shape=[whole, whole],
        scratch_shapes=[whole, whole, pltpu.SemaphoreType.DMA((2, STEPS))],
        compiler_params=limits,
    )(
        pltpu.with_memory_space_constraint(gradients, pltpu.HBM),
        pltpu.with_memory_space_constraint(momentum, pltpu.HBM),
    )


def in_parts(x):
    first = x.astype(jnp.bfloat16)
    rest = x - first.astype(jnp.float32)
    second = rest.astype(jnp.bfloat16)
    third = (rest - second.astype(jnp.float32)).astype(jnp.bfloat16)
    return first, second, third


def on_left(a):
    first, second, third = in_parts(a)
    return jnp.concatenate([first, first, second, second, first, third], axis=1)


def on_right(b):
    first, second, third = in_parts(b)
    return jnp.concatenate([first, second, first, second, third, first], axis=0)


def product(left, right):
    half = left.shape[0] // 2
    upper = jnp.dot(left[:half], right, preferred_element_type=jnp.float32)
    lower = jnp.dot(left[half:], right, preferred_element_type=jnp.float32)
    return jnp.concatenate([upper, lower], axis=0)


def polynomial(gram):
    side = gram.shape[-1]
    row = lax.broadcasted_iota(jnp.int32, (side, side), 0)
    col = lax.broadcasted_iota(jnp.int32, (side, side), 1)
    eye = jnp.where(row == col, 1.0, 0.0)
    scale = lax.rsqrt(jnp.sum(gram * eye, keepdims=True) + 1e-06)
    a = gram * (scale * scale)
    q = eye * scale
    for step in range(ITERS):
        square = product(on_left(a), on_right(a))
        p = 3.4445 * eye + (-4.775 * a + 2.0315 * square)
        left = on_left(p)
        if step + 1 == ITERS:
            return product(left, on_right(q))
        if step == 0:
            q = p * scale
            once = product(left, on_right(a))
        else:
            both = product(left, on_right(jnp.concatenate([a, q], axis=1)))
            once, q = both[:, :side], both[:, side:]
        a = product(left, on_right(once))


def update_body(x_ref, momentum_ref, out_ref, kept_ref, pieces_ref, written):
    keep = pltpu.make_async_copy(momentum_ref, kept_ref, written)
    keep.start()
    side = pieces_ref.shape[0] // 3
    wide = x_ref.shape[-1]
    parts = [(i, j) for i in range(x_ref.shape[1]) for j in range(x_ref.shape[4])]
    upper = lower = None
    for k, (i, j) in enumerate(parts):
        first, second, third = in_parts(x_ref[:, i, :, :, j].reshape(side, wide))
        pieces = jnp.concatenate([third, first, second], axis=0)
        pieces_ref[:, k * wide : (k + 1) * wide] = pieces
        half = pieces.shape[0] // 2
        sums = [
            lax.dot_general(rows, pieces[side:], (((1,), (1,)), ((), ())), preferred_element_type=jnp.float32)
            for rows in (pieces[:half], pieces[half:])
        ]
        upper = sums[0] if upper is None else upper + sums[0]
        lower = sums[1] if lower is None else lower + sums[1]
    sums = jnp.concatenate([upper, lower], axis=0)
    small = sums[:side, :side]
    small = (small + small.T) + sums[2 * side :, side:]
    small = small + (sums[2 * side :, :side] + sums[side : 2 * side, side:])
    left = on_left(polynomial(sums[side : 2 * side, :side] + small))
    for k, (i, j) in enumerate(parts):
        columns = slice(k * wide, (k + 1) * wide)
        large = pieces_ref[side:, columns]
        right = jnp.concatenate([large, large, pieces_ref[: 2 * side, columns]], axis=0)
        new = jnp.dot(left, right, preferred_element_type=jnp.float32)
        out_ref[:, i, :, :, j] = new.reshape(out_ref[:, i, :, :, j].shape)
    keep.wait()


def updated(x, momentum):
    _, halves, _, _, blocks, _, wide = x.shape
    columns = halves * blocks * wide
    return pl.pallas_call(
        update_body,
        in_specs=[pl.BlockSpec(memory_space=pltpu.VMEM), pl.BlockSpec(memory_space=pltpu.VMEM)],
        out_specs=[pl.BlockSpec(memory_space=pltpu.VMEM), pl.BlockSpec(memory_space=pltpu.HBM)],
        out_shape=[pltpu.VMEM(x.shape, x.dtype), pltpu.HBM(momentum.shape, momentum.dtype)],
        scratch_shapes=[
            pltpu.VMEM((3 * x.size // columns, columns), jnp.bfloat16),
            pltpu.SemaphoreType.DMA,
        ],
        compiler_params=limits,
    )(pltpu.with_memory_space_constraint(x, pltpu.VMEM), pltpu.with_memory_space_constraint(momentum, pltpu.VMEM))


def finish_body(weights_ref, back_ref, out_ref, new_ref, written):
    step = out_ref.shape[0] // STEPS
    copies = []
    for i in range(STEPS):
        rows = pl.ds(i * step, step)
        new_ref[rows] = weights_ref[rows] - learn_rate * back_ref[rows]
        copies.append(pltpu.make_async_copy(new_ref.at[rows], out_ref.at[rows], written.at[i]))
        copies[-1].start()
    for copy in copies:
        copy.wait()


def finished(weights, back):
    return pl.pallas_call(
        finish_body,
        in_specs=[pl.BlockSpec(memory_space=pltpu.VMEM), pl.BlockSpec(memory_space=pltpu.VMEM)],
        out_specs=pl.BlockSpec(memory_space=pltpu.HBM),
        out_shape=pltpu.HBM(weights.shape, weights.dtype),
        scratch_shapes=[pltpu.VMEM(weights.shape, weights.dtype), pltpu.SemaphoreType.DMA((STEPS,))],
        compiler_params=limits,
    )(pltpu.with_memory_space_constraint(weights, pltpu.VMEM), pltpu.with_memory_space_constraint(back, pltpu.VMEM))


def local(gradients, momentum, weights):
    direction, new_momentum = direction_of(gradients, momentum)
    mats, rows, wide = direction.shape
    sizes = tuple(lax.axis_size(axis) for axis in EVERY)
    x = lax.all_to_all(direction, EVERY, 0, 0, tiled=True)
    y, new_momentum = updated(x.reshape(*sizes, rows, wide), new_momentum)
    back = lax.all_to_all(y.reshape(mats, rows, wide), EVERY, 0, 0, tiled=True)
    return (finished(weights, back), new_momentum)


def solution(mesh):
    finer = Mesh(mesh.devices.reshape(4, 4, 2, 2, 4), (*SHARD, *MODEL))
    placed = P(None, SHARD, MODEL)
    return jax.shard_map(
        local,
        mesh=finer,
        in_specs=(placed, placed, placed),
        out_specs=(placed, placed),
        check_vma=False,
    )
```

```python
import jax
import jax.numpy as jnp
from jax import lax
from jax.experimental import pallas as pl
from jax.experimental.pallas import tpu as pltpu
from jax.sharding import Mesh
from jax.sharding import PartitionSpec as P

ITERS = 4
SHARD = ("shard_0", "shard_1", "shard_2")
MODEL = ("model_0", "model_1")
EVERY = (*SHARD, *MODEL)
ROWS = 32
PARTS = 8


def device_at(position):
    ring, core, y, x = position // 32, position // 16 % 2, position // 4 % 4, position % 4
    return ((ring % 4 * 4 + y) * 2 + core) * PARTS + ring // 4 * 4 + x


ORDER = [device_at(-131 * i % (ROWS * PARTS)) for i in range(ROWS * PARTS)]
PLACES = [[ORDER.index(row * PARTS + part) for row in range(ROWS)] for part in range(PARTS)]

STEPS = 8

hold_rate = 0.9
learn_rate = 0.8

limits = pltpu.CompilerParams(vmem_limit_bytes=16 << 20)


def direction_body(gradients_ref, momentum_ref, out_ref, new_ref, first_ref, second_ref, arrived):
    step = out_ref.shape[0] // STEPS

    def copies(i):
        rows = pl.ds(i * step, step)
        return (
            pltpu.make_async_copy(gradients_ref.at[rows], first_ref.at[rows], arrived.at[0, i]),
            pltpu.make_async_copy(momentum_ref.at[rows], second_ref.at[rows], arrived.at[1, i]),
        )

    for i in range(STEPS):
        for copy in copies(i):
            copy.start()
    for i in range(STEPS):
        for copy in copies(i):
            copy.wait()
        rows = pl.ds(i * step, step)
        gradients = first_ref[rows]
        new_momentum = hold_rate * second_ref[rows] + gradients
        new_ref[rows] = new_momentum
        out_ref[rows] = hold_rate * new_momentum + gradients


def direction_of(gradients, momentum):
    whole = pltpu.VMEM(gradients.shape, gradients.dtype)
    return pl.pallas_call(
        direction_body,
        in_specs=[pl.BlockSpec(memory_space=pltpu.HBM), pl.BlockSpec(memory_space=pltpu.HBM)],
        out_specs=[pl.BlockSpec(memory_space=pltpu.VMEM), pl.BlockSpec(memory_space=pltpu.VMEM)],
        out_shape=[whole, whole],
        scratch_shapes=[whole, whole, pltpu.SemaphoreType.DMA((2, STEPS))],
        compiler_params=limits,
    )(
        pltpu.with_memory_space_constraint(gradients, pltpu.HBM),
        pltpu.with_memory_space_constraint(momentum, pltpu.HBM),
    )


def in_parts(x):
    first = x.astype(jnp.bfloat16)
    rest = x - first.astype(jnp.float32)
    second = rest.astype(jnp.bfloat16)
    third = (rest - second.astype(jnp.float32)).astype(jnp.bfloat16)
    return first, second, third


def on_left(a):
    first, second, third = in_parts(a)
    return jnp.concatenate([first, first, second, second, first, third], axis=1)


def on_right(b):
    first, second, third = in_parts(b)
    return jnp.concatenate([first, second, first, second, third, first], axis=0)


def product(left, right):
    half = left.shape[0] // 2
    upper = jnp.dot(left[:half], right, preferred_element_type=jnp.float32)
    lower = jnp.dot(left[half:], right, preferred_element_type=jnp.float32)
    return jnp.concatenate([upper, lower], axis=0)


def polynomial(gram):
    side = gram.shape[-1]
    row = lax.broadcasted_iota(jnp.int32, (side, side), 0)
    col = lax.broadcasted_iota(jnp.int32, (side, side), 1)
    eye = jnp.where(row == col, 1.0, 0.0)
    scale = lax.rsqrt(jnp.sum(gram * eye, keepdims=True) + 1e-06)
    a = gram * (scale * scale)
    q = eye * scale
    for step in range(ITERS):
        square = product(on_left(a), on_right(a))
        p = 3.4445 * eye + (-4.775 * a + 2.0315 * square)
        left = on_left(p)
        if step + 1 == ITERS:
            return product(left, on_right(q))
        if step == 0:
            q = p * scale
            once = product(left, on_right(a))
        else:
            both = product(left, on_right(jnp.concatenate([a, q], axis=1)))
            once, q = both[:, :side], both[:, side:]
        a = product(left, on_right(once))


def update_body(x_ref, momentum_ref, out_ref, kept_ref, pieces_ref, written):
    keep = pltpu.make_async_copy(momentum_ref, kept_ref, written)
    keep.start()
    side = pieces_ref.shape[0] // 3
    wide = x_ref.shape[-1]
    height = x_ref.shape[1]
    upper = lower = None
    for k, places in enumerate(PLACES):
        first, second, third = in_parts(jnp.concatenate([x_ref[i] for i in places], axis=0))
        pieces = jnp.concatenate([third, first, second], axis=0)
        pieces_ref[:, k * wide : (k + 1) * wide] = pieces
        half = pieces.shape[0] // 2
        sums = [
            lax.dot_general(rows, pieces[side:], (((1,), (1,)), ((), ())), preferred_element_type=jnp.float32)
            for rows in (pieces[:half], pieces[half:])
        ]
        upper = sums[0] if upper is None else upper + sums[0]
        lower = sums[1] if lower is None else lower + sums[1]
    sums = jnp.concatenate([upper, lower], axis=0)
    small = sums[:side, :side]
    small = (small + small.T) + sums[2 * side :, side:]
    small = small + (sums[2 * side :, :side] + sums[side : 2 * side, side:])
    left = on_left(polynomial(sums[side : 2 * side, :side] + small))
    for k, places in enumerate(PLACES):
        columns = slice(k * wide, (k + 1) * wide)
        large = pieces_ref[side:, columns]
        right = jnp.concatenate([large, large, pieces_ref[: 2 * side, columns]], axis=0)
        new = jnp.dot(left, right, preferred_element_type=jnp.float32)
        for row, i in enumerate(places):
            out_ref[i] = new[row * height : (row + 1) * height]
    keep.wait()


def updated(x, momentum):
    columns = PARTS * x.shape[-1]
    return pl.pallas_call(
        update_body,
        in_specs=[pl.BlockSpec(memory_space=pltpu.VMEM), pl.BlockSpec(memory_space=pltpu.VMEM)],
        out_specs=[pl.BlockSpec(memory_space=pltpu.VMEM), pl.BlockSpec(memory_space=pltpu.HBM)],
        out_shape=[pltpu.VMEM(x.shape, x.dtype), pltpu.HBM(momentum.shape, momentum.dtype)],
        scratch_shapes=[
            pltpu.VMEM((3 * x.size // columns, columns), jnp.bfloat16),
            pltpu.SemaphoreType.DMA,
        ],
        compiler_params=limits,
    )(pltpu.with_memory_space_constraint(x, pltpu.VMEM), pltpu.with_memory_space_constraint(momentum, pltpu.VMEM))


def finish_body(weights_ref, back_ref, out_ref, new_ref, written):
    step = out_ref.shape[0] // STEPS
    copies = []
    for i in range(STEPS):
        rows = pl.ds(i * step, step)
        new_ref[rows] = weights_ref[rows] - learn_rate * back_ref[rows]
        copies.append(pltpu.make_async_copy(new_ref.at[rows], out_ref.at[rows], written.at[i]))
        copies[-1].start()
    for copy in copies:
        copy.wait()


def finished(weights, back):
    return pl.pallas_call(
        finish_body,
        in_specs=[pl.BlockSpec(memory_space=pltpu.VMEM), pl.BlockSpec(memory_space=pltpu.VMEM)],
        out_specs=pl.BlockSpec(memory_space=pltpu.HBM),
        out_shape=pltpu.HBM(weights.shape, weights.dtype),
        scratch_shapes=[pltpu.VMEM(weights.shape, weights.dtype), pltpu.SemaphoreType.DMA((STEPS,))],
        compiler_params=limits,
    )(pltpu.with_memory_space_constraint(weights, pltpu.VMEM), pltpu.with_memory_space_constraint(back, pltpu.VMEM))


def local(gradients, momentum, weights):
    direction, new_momentum = direction_of(gradients, momentum)
    x = lax.all_to_all(direction, EVERY, 0, 0, tiled=True, axis_index_groups=[ORDER])
    y, new_momentum = updated(x, new_momentum)
    back = lax.all_to_all(y, EVERY, 0, 0, tiled=True, axis_index_groups=[ORDER])
    return (finished(weights, back), new_momentum)


def solution(mesh):
    finer = Mesh(mesh.devices.reshape(4, 4, 2, 2, 4), (*SHARD, *MODEL))
    placed = P(None, SHARD, MODEL)
    return jax.shard_map(
        local,
        mesh=finer,
        in_specs=(placed, placed, placed),
        out_specs=(placed, placed),
        check_vma=False,
    )
```
